256 devices in a mesh: gx: 4 (over x), gy: 8 (over z_hi, y), gz: 8 (over z_lo, core).
Axes of the slice: x: 4, y: 4, z: 8 (z_hi: 2, z_lo: 4; z = z_hi * 4 + z_lo), core: 2. Of those that a mesh axis runs over, the one named last changes fastest.
Arguments:
- velocity: float32 [3, 128, 768, 2048], P(None, 'gx', 'gy', 'gz'), may hold values from -6 to 6
Outputs:
- magnitude: float32 [128, 768, 2048], P('gx', ('gy', 'gz'))
- level_one: float32 [64, 384, 1024], P('gx', 'gy')
- level_two: float32 [32, 192, 512], P('gx', 'gy')
- level_three: float32 [16, 96, 256], P('gx', 'gy')
- level_four: float32 [8, 48, 128], P('gx', 'gy')
- level_five: float32 [4, 24, 64], P('gx', 'gy')
The draws below stay inside these ranges and needn't reach their ends.
All inputs are finite; a program needn't handle non-finite values.
Results may differ from the reference program's by a relative error of at most 0.000075.
Values sent between devices are 32-bit elements; how exact they have to be, the bound alone decides.
A program may use at most 256 MiB of HBM per device.

```python
import jax
import jax.numpy as jnp
from jax import lax

NX = 128
NY = 768
NZ = 2048


def shard_levels(stream_key, extent, cuts, least, top_value):
    loudness, own = 1.0, jax.random.fold_in(stream_key, 6)
    for axis_at, blocks in cuts:
        steps = jnp.exp(jax.random.uniform(jax.random.fold_in(own, axis_at), (blocks,), jnp.float32, least / len(cuts), top_value / len(cuts)))
        loudness = loudness * jnp.repeat(steps, extent[axis_at] // blocks).reshape([-1 if axis == axis_at else 1 for axis in range(len(extent))])
    return loudness


def normal_values(own_key, extent, scale, limit, split=(), held_as=jnp.bfloat16):
    level = shard_levels(own_key, extent, split, -0.22, 0.18) if split else 1.0
    array = jax.random.normal(own_key, extent, jnp.float32) * scale * level
    return jnp.minimum(jnp.maximum(array, -limit), limit).astype(held_as)


def setup_inputs(seed: int = 0) -> dict:
    streams_of = jax.random.split(jax.random.key(seed), 2)
    velocity = normal_values(streams_of[0], (3, NX, NY, NZ), 1.0, 6.0, ((1, 4), (2, 8), (3, 8)), jnp.float32)
    return {"velocity": velocity}


def central(field, axis):
    return (jnp.roll(field, -1, axis) - jnp.roll(field, 1, axis)) * 0.5

def pooled(field):
    rows, cols, depth = field.shape
    blocks = field.reshape(rows // 2, 2, cols // 2, 2, depth // 2, 2)
    return lax.optimization_barrier(jnp.mean(blocks, axis=(1, 3, 5)))

def reference(velocity):
    speed_u = velocity[0]
    speed_v = velocity[1]
    speed_w = velocity[2]
    curl_first = central(speed_w, 1) - central(speed_v, 2)
    curl_second = central(speed_u, 2) - central(speed_w, 0)
    curl_third = central(speed_v, 0) - central(speed_u, 1)
    magnitude = jnp.sqrt(1.0 + curl_first * curl_first + curl_second * curl_second + curl_third * curl_third)
    level_one = pooled(magnitude)
    level_two = pooled(level_one)
    level_three = pooled(level_two)
    level_four = pooled(level_three)
    level_five = pooled(level_four)
    return (magnitude, level_one, level_two, level_three, level_four, level_five)
```

```python
import functools

import jax
import jax.numpy as jnp
from jax import lax
from jax.experimental import pallas as pl
from jax.experimental.pallas import tpu as pltpu
from jax.sharding import PartitionSpec as P

F32 = jnp.float32
GROUP = 8
CHIPS = 4
ORDER = (1, 2, 0, 3)
U, V, W = (0, 1, 2)


def pairing():
    upper = lax.broadcasted_iota(jnp.int32, (256, 128), 0) // 2
    lower = lax.broadcasted_iota(jnp.int32, (256, 128), 1)
    return (upper == lower).astype(F32)


def lane_pairs(value, pair):
    return jnp.dot(value, pair, precision=lax.Precision.HIGHEST, preferred_element_type=F32)


def flip(index, mask):
    bits = [(index // w) % 2 for w in (1, 2, 4)]
    bits = [1 - b if (mask >> i) % 2 else b for i, b in enumerate(bits)]
    return bits[0] + 2 * bits[1] + 4 * bits[2]


def exchange(
    vel_hbm, pencil, level, vel, planes, block, own, halves, edge_out, edge_in, row_out, row_in,
    load_sem, x_sem, y_sem, z_sem, a2a_send, a2a_recv, level_send, level_recv, own_sem, peer_sem,
):
    gx, gy, gz = (lax.axis_index("gx"), lax.axis_index("gy"), lax.axis_index("gz"))
    chip, core = (gz // 2, gz % 2)
    x_sides = [{"gx": (gx + 3) % 4}, {"gx": (gx + 1) % 4}]
    y_sides = [{"gy": (gy + 7) % 8}, {"gy": (gy + 1) % 8}]
    z_sides = [{"gz": (gz + 7) % 8}, {"gz": (gz + 1) % 8}]

    loads = [
        pltpu.make_async_copy(vel_hbm.at[c], vel.at[c, 1:33], load_sem.at[c]) for c in (U, V, W)
    ]
    for copy in loads:
        copy.start()

    barrier = pltpu.get_barrier_semaphore()
    for mask in range(1, 8):
        pl.semaphore_signal(barrier, inc=1, device_id={"gz": flip(gz, mask)})
    for side in x_sides + y_sides:
        pl.semaphore_signal(barrier, inc=1, device_id=side)

    row = lax.broadcasted_iota(jnp.int32, (96, 128), 0)
    lane = lax.broadcasted_iota(jnp.int32, (96, 128), 1)

    loads[U].wait()
    loads[V].wait()

    def pack_edges(x, carry):
        first, last = carry
        for comp in (U, V):
            at = comp * 32 + x
            first = jnp.where(lane == at, pltpu.roll(vel[comp, x + 1, :, 0:128], at, 1), first)
            last = jnp.where(lane == at, pltpu.roll(vel[comp, x + 1, :, 128:256], at + 1, 1), last)
        return first, last

    zero = jnp.zeros((96, 128), F32)
    first, last = lax.fori_loop(0, 32, pack_edges, (zero, zero))
    edge_out[0] = first
    edge_out[1] = last
    loads[W].wait()

    def pack_rows(x, carry):
        for spot, comp in enumerate((U, W)):
            for half in (0, 1):
                lanes = slice(half * 128, half * 128 + 128)
                row_out[0, spot, x, half : half + 1, :] = vel[comp, x + 1, 0:1, lanes]
                row_out[1, spot, x, half : half + 1, :] = vel[comp, x + 1, 95:96, lanes]
        return carry

    lax.fori_loop(0, 32, pack_rows, 0)
    pl.semaphore_wait(barrier, 11)

    halos = []
    for side in (0, 1):
        halos.append(
            pltpu.make_async_remote_copy(
                edge_out.at[side], edge_in.at[1 - side], z_sem.at[0, side], z_sem.at[1, 1 - side],
                device_id=z_sides[side],
            )
        )
        halos.append(
            pltpu.make_async_remote_copy(
                row_out.at[side], row_in.at[1 - side], y_sem.at[0, side], y_sem.at[1, 1 - side],
                device_id=y_sides[side],
            )
        )
        halos.append(
            pltpu.make_async_remote_copy(
                vel.at[1:3, 32 * side - side + 1], vel.at[1:3, 33 - 33 * side],
                x_sem.at[0, side], x_sem.at[1, 1 - side], device_id=x_sides[side],
            )
        )
    for copy in halos:
        copy.start()
    for copy in (halos[0], halos[3], halos[1], halos[4]):
        copy.wait_recv()

    pair = pairing()

    def second_diff(comp, spot, x, half):
        lanes = slice(half * 128, half * 128 + 128)
        value = vel[comp, x + 1, :, lanes]
        before = row_in[0, spot, x, half : half + 1, :]
        after = row_in[1, spot, x, half : half + 1, :]
        ahead = jnp.where(row == 95, after, pltpu.roll(value, 95, 0))
        behind = jnp.where(row == 0, before, pltpu.roll(value, 1, 0))
        return ahead - behind

    def third_diff(comp, x, half):
        low = vel[comp, x + 1, :, 0:128]
        high = vel[comp, x + 1, :, 128:256]
        at = comp * 32 + x
        if half == 0:
            into_first = pltpu.roll(edge_in[0], (128 - at) % 128, 1)
            into_last, here = (pltpu.roll(high, 127, 1), low)
        else:
            into_last = pltpu.roll(edge_in[1], 127 - at, 1)
            into_first, here = (pltpu.roll(low, 1, 1), high)
        ahead = jnp.where(lane == 127, into_last, pltpu.roll(here, 127, 1))
        behind = jnp.where(lane == 0, into_first, pltpu.roll(here, 1, 1))
        return ahead - behind

    def first_diff(comp, x, half):
        lanes = slice(half * 128, half * 128 + 128)
        return vel[comp, x + 2, :, lanes] - vel[comp, x, :, lanes]

    def level_copy(source, part, origin, kind, target):
        rows = pl.ds(part * 4, 4)
        lanes = pl.ds(pl.multiple_of(origin * 128, 128), 128)
        return pltpu.make_async_remote_copy(
            own.at[rows] if source is None else level.at[rows, :, lanes],
            level.at[rows, :, lanes],
            level_send.at[kind, origin // 2, part],
            level_recv.at[origin, part],
            device_id={"gz": target},
        )

    def own_copy(part):
        lanes = pl.ds(pl.multiple_of(gz * 128, 128), 128)
        return pltpu.make_async_copy(
            own.at[pl.ds(part * 4, 4)], level.at[pl.ds(part * 4, 4), :, lanes], own_sem.at[0, part]
        )

    def piece_copy(mask, part):
        target = flip(gz, mask)
        rows = pl.ds(part * 8, 8)
        lanes = pl.ds(pl.multiple_of(gz * 256, 256), 256)
        source = block.at[pl.ds(target * 12, 12), rows, :]
        if mask == 0:
            return pltpu.make_async_copy(source, pencil.at[:, rows, lanes], own_sem.at[1, part])
        return pltpu.make_async_remote_copy(
            source, pencil.at[:, rows, lanes], a2a_send.at[mask, part], a2a_recv.at[mask, part],
            device_id={"gz": target},
        )

    for part in ORDER:
        if part == 0:
            halos[2].wait_recv()
            halos[5].wait_recv()

        def one_plane(i, carry):
            x = part * 8 + i
            for half in (0, 1):
                one = second_diff(W, 1, x, half) - third_diff(V, x, half)
                total = one * one
                two = third_diff(U, x, half) - first_diff(W, x, half)
                total = total + two * two
                three = first_diff(V, x, half) - second_diff(U, 0, x, half)
                total = total + three * three
                planes[i, :, half * 128 : half * 128 + 128] = jnp.sqrt(1.0 + 0.25 * total)
            return carry

        lax.fori_loop(0, GROUP, one_plane, 0)

        def turn(y, carry):
            rows = pl.ds(pl.multiple_of(y * 8, 8), 8)
            for half in (0, 1):
                lanes = slice(half * 128, half * 128 + 128)
                block[rows, part * 8 : part * 8 + 8, lanes] = jnp.swapaxes(
                    planes[:, rows, lanes], 0, 1
                )
            return carry

        lax.fori_loop(0, 12, turn, 0)

        for j in range(4):
            halves[...] = lane_pairs(planes[2 * j] + planes[2 * j + 1], pair)
            even = halves[pl.ds(0, 48, stride=2), :]
            odd = halves[pl.ds(1, 48, stride=2), :]
            own[part * 4 + j] = (even + odd) * 0.125

        @pl.when(chip < 3)
        def _():
            level_copy(None, part, gz, 0, gz + 2).start()

        @pl.when(chip > 0)
        def _():
            level_copy(None, part, gz, 1, gz - 2).start()

        level_copy(None, part, gz, 2, flip(gz, 1)).start()
        for mask in (6, 7, 4, 5, 2, 3, 1, 0):
            piece_copy(mask, part).start()
        own_copy(part).start()

    for hop in (1, 2, 3):
        for part in ORDER:

            @pl.when(chip >= hop)
            def _():
                origin = gz - 2 * hop
                level_copy(None, part, origin, 0, gz).wait_recv()

                @pl.when(chip < 3)
                def _():
                    level_copy(level, part, origin, 0, gz + 2).start()

                level_copy(level, part, origin, 2, flip(gz, 1)).start()

            @pl.when(chip + hop < 4)
            def _():
                origin = gz + 2 * hop
                level_copy(None, part, origin, 1, gz).wait_recv()

                @pl.when(chip > 0)
                def _():
                    level_copy(level, part, origin, 1, gz - 2).start()

                level_copy(level, part, origin, 2, flip(gz, 1)).start()

    for part in ORDER:
        own_copy(part).wait()
        piece_copy(0, part).wait()
        for mask in range(1, 8):
            piece_copy(mask, part).wait()
        for q in range(CHIPS):
            other = 2 * q + 1 - core
            mine = 2 * q + core
            level_copy(level, part, other, 2, flip(gz, 1)).wait_recv()
            level_copy(level, part, mine, 2, flip(gz, 1)).wait_send()

            @pl.when((q <= chip) & (chip < 3))
            def _():
                level_copy(level, part, mine, 0, gz).wait_send()

            @pl.when((q >= chip) & (chip > 0))
            def _():
                level_copy(level, part, mine, 1, gz).wait_send()

    for copy in halos:
        copy.wait_send()


def finish(
    pencil, level, mag_out, one_out, two_out, three_out, four_out, five_out,
    two_half, three_half, four_half, five_half, three_at, four_at, sems,
):
    copies = [
        pltpu.make_async_copy(pencil, mag_out, sems.at[0]),
        pltpu.make_async_copy(level, one_out, sems.at[1]),
    ]
    for copy in copies:
        copy.start()
    pair = pairing()

    def step(low, high, half, rows, lanes):
        summed = low + high
        if lanes >= 256:
            for s in range(lanes // 256):
                half[0:rows, s * 128 : s * 128 + 128] = lane_pairs(
                    summed[:, s * 256 : s * 256 + 256], pair
                )
        else:
            half[0:rows, 0:64] = lane_pairs(summed, pair[0:128, 0:64])
        width = lanes // 2
        even = half[pl.ds(0, rows // 2, stride=2), 0:width]
        odd = half[pl.ds(1, rows // 2, stride=2), 0:width]
        return (even + odd) * 0.125

    for i in range(8):
        for s in range(4):
            summed = level[2 * i, :, s * 256 : s * 256 + 256] + level[2 * i + 1, :, s * 256 : s * 256 + 256]
            two_half[s, :, :] = lane_pairs(summed, pair)
            even = two_half[s, pl.ds(0, 24, stride=2), :]
            odd = two_half[s, pl.ds(1, 24, stride=2), :]
            two_out[i, :, s * 128 : s * 128 + 128] = (even + odd) * 0.125
    for i in range(4):
        for s in range(2):
            lanes = slice(s * 256, s * 256 + 256)
            three_half[...] = lane_pairs(two_out[2 * i, :, lanes] + two_out[2 * i + 1, :, lanes], pair)
            even = three_half[pl.ds(0, 12, stride=2), :]
            odd = three_half[pl.ds(1, 12, stride=2), :]
            value = (even + odd) * 0.125
            three_at[i, :, s * 128 : s * 128 + 128] = value
            for r in range(12):
                three_out[r, i : i + 1, s * 128 : s * 128 + 128] = value[r : r + 1]
    for i in range(2):
        four_half[...] = lane_pairs(three_at[2 * i] + three_at[2 * i + 1], pair)
        value = (four_half[pl.ds(0, 6, stride=2), :] + four_half[pl.ds(1, 6, stride=2), :]) * 0.125
        four_at[i] = value
        for r in range(6):
            four_out[r, i : i + 1, :] = value[r : r + 1]
    five_half[...] = lane_pairs(four_at[0] + four_at[1], pair[0:128, :])
    value = (five_half[pl.ds(0, 3, stride=2), :] + five_half[pl.ds(1, 3, stride=2), :]) * 0.125
    for r in range(3):
        five_out[r] = value[r : r + 1, 0:64]
    for copy in copies:
        copy.wait()


def on_device(velocity):
    dma, vmem = (pltpu.SemaphoreType.DMA, pltpu.VMEM)
    pencil, level = pl.pallas_call(
        exchange,
        name="exchange",
        out_shape=(vmem((12, 32, 2048), F32), vmem((16, 48, 1024), F32)),
        in_specs=[pl.BlockSpec(memory_space=pl.ANY)],
        out_specs=(pl.BlockSpec(memory_space=vmem), pl.BlockSpec(memory_space=vmem)),
        scratch_shapes=[
            vmem((3, 34, 96, 256), F32),
            vmem((8, 96, 256), F32),
            vmem((96, 32, 256), F32),
            vmem((16, 48, 128), F32),
            vmem((96, 128), F32),
            vmem((2, 96, 128), F32),
            vmem((2, 96, 128), F32),
            vmem((2, 2, 32, 2, 128), F32),
            vmem((2, 2, 32, 2, 128), F32),
            dma((3,)),
            dma((2, 2)),
            dma((2, 2)),
            dma((2, 2)),
            dma((8, 4)),
            dma((8, 4)),
            dma((3, 4, 4)),
            dma((8, 4)),
            dma((2, 4)),
            dma((1,)),
        ],
        compiler_params=pltpu.CompilerParams(
            collective_id=0, has_side_effects=True, vmem_limit_bytes=48 * 1024 * 1024
        ),
    )(velocity)
    any_space = pl.BlockSpec(memory_space=pl.ANY)
    local = pl.BlockSpec(memory_space=vmem)
    mag, one, two, three, four, five = pl.pallas_call(
        finish,
        name="finish",
        out_shape=(
            jax.ShapeDtypeStruct((12, 32, 2048), F32),
            jax.ShapeDtypeStruct((16, 48, 1024), F32),
            jax.ShapeDtypeStruct((8, 24, 512), F32),
            jax.ShapeDtypeStruct((12, 4, 256), F32),
            jax.ShapeDtypeStruct((6, 2, 128), F32),
            jax.ShapeDtypeStruct((3, 1, 64), F32),
        ),
        in_specs=[local, local],
        out_specs=(any_space, any_space, local, local, local, local),
        scratch_shapes=[
            vmem((4, 48, 128), F32),
            vmem((24, 128), F32),
            vmem((12, 128), F32),
            vmem((6, 128), F32),
            vmem((4, 12, 256), F32),
            vmem((2, 6, 128), F32),
            dma((2,)),
        ],
    )(pencil, level)
    swap = lambda value: jnp.swapaxes(value, 0, 1)
    return swap(mag), one, two, swap(three), swap(four), swap(five)


def solution(mesh):
    in_specs = (P(None, "gx", "gy", "gz"),)
    out_specs = (
        P("gx", ("gy", "gz"), None),
        P("gx", "gy", None),
        P("gx", "gy", None),
        P("gx", "gy", None),
        P("gx", "gy", None),
        P("gx", "gy", None),
    )
    return jax.shard_map(
        on_device, mesh=mesh, in_specs=in_specs, out_specs=out_specs, check_vma=False
    )
```

```python
import functools

import jax
import jax.numpy as jnp
from jax import lax
from jax.experimental import pallas as pl
from jax.experimental.pallas import tpu as pltpu
from jax.sharding import PartitionSpec as P

F32 = jnp.float32
GROUP = 8
ORDER = (1, 2, 0, 3)
U, V, W = (0, 1, 2)


def pairing():
    upper = lax.broadcasted_iota(jnp.int32, (256, 128), 0) // 2
    lower = lax.broadcasted_iota(jnp.int32, (256, 128), 1)
    return (upper == lower).astype(F32)


def lane_pairs(value, pair):
    return jnp.dot(value, pair, precision=lax.Precision.HIGHEST, preferred_element_type=F32)


def flip(index, mask):
    bits = [(index // w) % 2 for w in (1, 2, 4)]
    bits = [1 - b if (mask >> i) % 2 else b for i, b in enumerate(bits)]
    return bits[0] + 2 * bits[1] + 4 * bits[2]


def exchange(
    vel_hbm, pencil, level, vel, planes, block, own, halves, thirds, edge_out, edge_in, row_out,
    row_in, far, load_sem, x_sem, y_sem, z_sem, a2a_send, a2a_recv, send_sem, level_recv, far_recv,
    own_sem,
):
    gx, gy, gz = (lax.axis_index("gx"), lax.axis_index("gy"), lax.axis_index("gz"))
    half = gz // 4
    x_sides = [{"gx": (gx + 3) % 4}, {"gx": (gx + 1) % 4}]
    y_sides = [{"gy": (gy + 7) % 8}, {"gy": (gy + 1) % 8}]
    z_sides = [{"gz": (gz + 7) % 8}, {"gz": (gz + 1) % 8}]

    def load(comp, part):
        return pltpu.make_async_copy(
            vel_hbm.at[comp, pl.ds(part * 8, 8)],
            vel.at[comp, pl.ds(part * 8 + 1, 8), 8:104],
            load_sem.at[comp, part],
        )

    for part in range(4):
        load(U, part).start()
        load(V, part).start()
    for part in range(4):
        load(W, part).start()

    barrier = pltpu.get_barrier_semaphore()
    for mask in range(1, 8):
        pl.semaphore_signal(barrier, inc=1, device_id={"gz": flip(gz, mask)})
    for side in x_sides + y_sides:
        pl.semaphore_signal(barrier, inc=1, device_id=side)

    lane = lax.broadcasted_iota(jnp.int32, (96, 128), 1)

    def pack_edges(x, carry):
        first, last = carry
        for comp in (U, V):
            at = comp * 32 + x
            low, high = (vel[comp, x + 1, 8:104, 0:128], vel[comp, x + 1, 8:104, 128:256])
            first = jnp.where(lane == at, pltpu.roll(low, at, 1), first)
            last = jnp.where(lane == at, pltpu.roll(high, at + 1, 1), last)
        return first, last

    edges = (jnp.zeros((96, 128), F32), jnp.zeros((96, 128), F32))
    for part in range(4):
        load(U, part).wait()
        load(V, part).wait()
        edges = lax.fori_loop(part * 8, part * 8 + 8, pack_edges, edges)
    edge_out[0] = edges[0]
    edge_out[1] = edges[1]

    z_halos, y_halos, x_halos = ([], [], [])
    for side in (0, 1):
        z_halos.append(
            pltpu.make_async_remote_copy(
                edge_out.at[side], edge_in.at[1 - side], z_sem.at[0, side], z_sem.at[1, 1 - side],
                device_id=z_sides[side],
            )
        )
        y_halos.append(
            pltpu.make_async_remote_copy(
                row_out.at[side], row_in.at[1 - side], y_sem.at[0, side], y_sem.at[1, 1 - side],
                device_id=y_sides[side],
            )
        )
        x_halos.append(
            pltpu.make_async_remote_copy(
                vel.at[1:3, 31 * side + 1, 8:104], vel.at[1:3, 33 - 33 * side, 8:104],
                x_sem.at[0, side], x_sem.at[1, 1 - side], device_id=x_sides[side],
            )
        )
    pl.semaphore_wait(barrier, 11)
    for copy in z_halos:
        copy.start()

    def pack_rows(x, carry):
        for spot, comp in enumerate((U, W)):
            for h in (0, 1):
                lanes = slice(h * 128, h * 128 + 128)
                row_out[0, spot, x, h : h + 1, :] = vel[comp, x + 1, 8:9, lanes]
                row_out[1, spot, x, h : h + 1, :] = vel[comp, x + 1, 103:104, lanes]
        return carry

    for part in range(4):
        load(W, part).wait()
    lax.fori_loop(0, 32, pack_rows, 0)
    for copy in y_halos + x_halos:
        copy.start()
    for copy in z_halos:
        copy.wait_recv()

    pair = pairing()

    def magnitude_rows(x, start, count):
        rows = pl.ds(pl.multiple_of(start, 8), count)
        inner = pl.ds(pl.multiple_of(start + 8, 8), count)
        outer = pl.ds(pl.multiple_of(start, 8), count + 16)
        column = lax.broadcasted_iota(jnp.int32, (count, 128), 1)

        for h in (0, 1):
            lanes = slice(h * 128, h * 128 + 128)

            def second_diff(comp):
                value = vel[comp, x + 1, outer, lanes]
                ahead = pltpu.roll(value, count + 15, 0)
                behind = pltpu.roll(value, 1, 0)
                return (ahead - behind)[8 : 8 + count]

            def third_diff(comp):
                low = vel[comp, x + 1, inner, 0:128]
                high = vel[comp, x + 1, inner, 128:256]
                at = comp * 32 + x
                if h == 0:
                    into_first = pltpu.roll(edge_in[0, rows, :], (128 - at) % 128, 1)
                    into_last, here = (pltpu.roll(high, 127, 1), low)
                else:
                    into_last = pltpu.roll(edge_in[1, rows, :], 127 - at, 1)
                    into_first, here = (pltpu.roll(low, 1, 1), high)
                ahead = jnp.where(column == 127, into_last, pltpu.roll(here, 127, 1))
                behind = jnp.where(column == 0, into_first, pltpu.roll(here, 1, 1))
                return ahead - behind

            def first_diff(comp):
                return vel[comp, x + 2, inner, lanes] - vel[comp, x, inner, lanes]

            one = second_diff(W) - third_diff(V)
            total = one * one
            two = third_diff(U) - first_diff(W)
            total = total + two * two
            three = first_diff(V) - second_diff(U)
            total = total + three * three
            planes[x, rows, lanes] = jnp.sqrt(1.0 + 0.25 * total)

    def make_rows(part, start, count):
        def one_plane(i, carry):
            magnitude_rows(part * 8 + i, start, count)
            return carry

        lax.fori_loop(0, GROUP, one_plane, 0)

        def turn(y, carry):
            rows = pl.ds(pl.multiple_of(start + y * 8, 8), 8)
            for h in (0, 1):
                lanes = slice(h * 128, h * 128 + 128)
                block[rows, part * 8 : part * 8 + 8, lanes] = jnp.swapaxes(
                    planes[part * 8 : part * 8 + 8, rows, lanes], 0, 1
                )
            return carry

        lax.fori_loop(0, count // 8, turn, 0)

    def piece_copy(mask, part):
        target = flip(gz, mask)
        rows = pl.ds(part * 8, 8)
        lanes = pl.ds(pl.multiple_of(gz * 256, 256), 256)
        source = block.at[pl.ds(target * 12, 12), rows, :]
        if mask == 0:
            return pltpu.make_async_copy(source, pencil.at[:, rows, lanes], own_sem.at[1, part])
        return pltpu.make_async_remote_copy(
            source, pencil.at[:, rows, lanes], a2a_send.at[mask, part], a2a_recv.at[mask, part],
            device_id={"gz": target},
        )

    def send_pieces(masks, part, inner):
        for mask in masks:
            target = flip(gz, mask)
            interior = (target > 0) & (target < 7)

            @pl.when(interior if inner else jnp.logical_not(interior))
            def _():
                piece_copy(mask, part).start()

    FAR, NEAR = ((6, 7, 4, 5), (2, 3, 1, 0))
    far_start, near_start = ((1 - half) * 48, half * 48)

    def level_copy(kind, part, origin, target, mine=False):
        every = kind < 3
        first = 0 if every else pl.multiple_of((origin // 4) * 24, 8)
        rows = pl.ds(first, 48 if every else 24)
        parts = pl.ds(part * 4, 4)
        lanes = pl.ds(pl.multiple_of(origin * 128, 128), 128)
        place = level.at[parts, rows, lanes]
        return pltpu.make_async_remote_copy(
            own.at[parts, rows] if mine else place, place,
            send_sem.at[kind, part], level_recv.at[origin, part], device_id={"gz": target},
        )

    def far_copy(kind, part, origin, target):
        place = far.at[origin % 4, pl.ds(part * 4, 4)]
        return pltpu.make_async_remote_copy(
            place, place, send_sem.at[kind, part], far_recv.at[origin % 4, part],
            device_id={"gz": target},
        )

    def own_copy(part):
        lanes = pl.ds(pl.multiple_of(gz * 128, 128), 128)
        return pltpu.make_async_copy(
            own.at[pl.ds(part * 4, 4)], level.at[pl.ds(part * 4, 4), :, lanes], own_sem.at[0, part]
        )

    mate, beside, across, past = (flip(gz, 1), flip(gz, 2), flip(gz, 6), flip(gz, 4))

    for part in ORDER:
        if part == 0:
            for copy in x_halos:
                copy.wait_recv()
        make_rows(part, far_start, 48)
        if part != 3:
            send_pieces(FAR, part, True)
        make_rows(part, near_start, 48)
        if part != 3:
            send_pieces(NEAR, part, True)

    for copy in y_halos:
        copy.wait_recv()

    def fill_rows(x, carry):
        for spot, comp in enumerate((U, W)):
            for h in (0, 1):
                lanes = slice(h * 128, h * 128 + 128)
                vel[comp, x + 1, 7:8, lanes] = row_in[0, spot, x, h : h + 1, :]
                vel[comp, x + 1, 104:105, lanes] = row_in[1, spot, x, h : h + 1, :]
        return carry

    lax.fori_loop(0, 32, fill_rows, 0)
    for part in ORDER:
        make_rows(part, 0, 8)
        make_rows(part, 88, 8)
        for j in range(part * 4, part * 4 + 4):
            halves[...] = lane_pairs(planes[2 * j] + planes[2 * j + 1], pair)
            even = halves[pl.ds(0, 48, stride=2), :]
            odd = halves[pl.ds(1, 48, stride=2), :]
            own[j] = (even + odd) * 0.125
        level_copy(3, part, gz, across, True).start()
        level_copy(1, part, gz, beside, True).start()
        level_copy(0, part, gz, mate, True).start()
        own_copy(part).start()
    for part in ORDER:
        send_pieces(FAR + NEAR, part, False)
        if part == 3:
            send_pieces(FAR + NEAR, part, True)

    def pass_far(part):
        for mask in FAR:
            piece_copy(mask, part).wait_recv()
        parts = pl.ds(part * 8, 8)
        for s in range(4):
            lanes = pl.ds(pl.multiple_of((1 - half) * 1024 + s * 256, 256), 256)
            rows = [pencil[2 * r, parts, lanes] + pencil[2 * r + 1, parts, lanes] for r in range(6)]
            thirds[s] = lane_pairs(jnp.concatenate(rows, axis=0), pair)
            for j in range(4):
                even = thirds[s, pl.ds(2 * j, 6, stride=8), :]
                odd = thirds[s, pl.ds(2 * j + 1, 6, stride=8), :]
                far[gz % 4, part * 4 + j, 0:6, s * 128 : s * 128 + 128] = (even + odd) * 0.125
        far_copy(8, part, gz, beside).start()
        far_copy(7, part, gz, mate).start()

    def pass_level(part):
        level_copy(3, part, across, across).wait_recv()
        level_copy(4, part, across, beside).start()
        level_copy(5, part, across, mate).start()

    for part in ORDER:
        level_copy(1, part, beside, beside).wait_recv()
        level_copy(2, part, beside, mate).start()
    for part in ORDER[:3]:
        pass_far(part)
    for part in ORDER:
        pass_level(part)
    for part in ORDER[:3]:
        far_copy(8, part, beside, beside).wait_recv()
        far_copy(9, part, beside, mate).start()
    for part in ORDER:
        level_copy(4, part, past, beside).wait_recv()
        level_copy(6, part, past, mate).start()
    pass_far(3)
    far_copy(8, 3, beside, beside).wait_recv()
    far_copy(9, 3, beside, mate).start()

    for part in ORDER:
        own_copy(part).wait()
        piece_copy(0, part).wait()
        for mask in range(1, 8):
            piece_copy(mask, part).wait_send()
        for mask in (1, 2, 3):
            piece_copy(mask, part).wait_recv()
        level_copy(0, part, mate, mate).wait_recv()
        level_copy(2, part, flip(gz, 3), mate).wait_recv()
        level_copy(5, part, flip(gz, 7), mate).wait_recv()
        level_copy(6, part, flip(gz, 5), mate).wait_recv()
        far_copy(7, part, mate, mate).wait_recv()
        far_copy(9, part, flip(gz, 3), mate).wait_recv()

    for side in (0, 1):

        @pl.when(half == side)
        def _():
            for d in range(4):
                rows = slice(side * 24 + d * 6, side * 24 + d * 6 + 6)
                lanes = slice((1 - side) * 512, (1 - side) * 512 + 512)

                def place_rows(j, carry):
                    level[j, rows, lanes] = far[d, j, 0:6, :]
                    return carry

                lax.fori_loop(0, 16, place_rows, 0)

    for part in ORDER:
        level_copy(0, part, gz, mate).wait_send()
        level_copy(1, part, gz, beside).wait_send()
        level_copy(2, part, beside, mate).wait_send()
        level_copy(3, part, gz, across).wait_send()
        level_copy(4, part, across, beside).wait_send()
        level_copy(5, part, across, mate).wait_send()
        level_copy(6, part, past, mate).wait_send()
        far_copy(7, part, gz, mate).wait_send()
        far_copy(8, part, gz, beside).wait_send()
        far_copy(9, part, beside, mate).wait_send()
    for copy in z_halos + y_halos + x_halos:
        copy.wait_send()


def finish(
    pencil, level, mag_out, one_out, two_out, three_out, four_out, five_out,
    two_half, three_half, four_half, five_half, three_at, four_at, sems,
):
    copies = [
        pltpu.make_async_copy(pencil, mag_out, sems.at[0]),
        pltpu.make_async_copy(level, one_out, sems.at[1]),
    ]
    for copy in copies:
        copy.start()
    pair = pairing()

    def step(low, high, half, rows, lanes):
        summed = low + high
        if lanes >= 256:
            for s in range(lanes // 256):
                half[0:rows, s * 128 : s * 128 + 128] = lane_pairs(
                    summed[:, s * 256 : s * 256 + 256], pair
                )
        else:
            half[0:rows, 0:64] = lane_pairs(summed, pair[0:128, 0:64])
        width = lanes // 2
        even = half[pl.ds(0, rows // 2, stride=2), 0:width]
        odd = half[pl.ds(1, rows // 2, stride=2), 0:width]
        return (even + odd) * 0.125

    for i in range(8):
        for s in range(4):
            summed = level[2 * i, :, s * 256 : s * 256 + 256] + level[2 * i + 1, :, s * 256 : s * 256 + 256]
            two_half[s, :, :] = lane_pairs(summed, pair)
            even = two_half[s, pl.ds(0, 24, stride=2), :]
            odd = two_half[s, pl.ds(1, 24, stride=2), :]
            two_out[i, :, s * 128 : s * 128 + 128] = (even + odd) * 0.125
    for i in range(4):
        for s in range(2):
            lanes = slice(s * 256, s * 256 + 256)
            three_half[...] = lane_pairs(two_out[2 * i, :, lanes] + two_out[2 * i + 1, :, lanes], pair)
            even = three_half[pl.ds(0, 12, stride=2), :]
            odd = three_half[pl.ds(1, 12, stride=2), :]
            value = (even + odd) * 0.125
            three_at[i, :, s * 128 : s * 128 + 128] = value
            for r in range(12):
                three_out[r, i : i + 1, s * 128 : s * 128 + 128] = value[r : r + 1]
    for i in range(2):
        four_half[...] = lane_pairs(three_at[2 * i] + three_at[2 * i + 1], pair)
        value = (four_half[pl.ds(0, 6, stride=2), :] + four_half[pl.ds(1, 6, stride=2), :]) * 0.125
        four_at[i] = value
        for r in range(6):
            four_out[r, i : i + 1, :] = value[r : r + 1]
    five_half[...] = lane_pairs(four_at[0] + four_at[1], pair[0:128, :])
    value = (five_half[pl.ds(0, 3, stride=2), :] + five_half[pl.ds(1, 3, stride=2), :]) * 0.125
    for r in range(3):
        five_out[r] = value[r : r + 1, 0:64]
    for copy in copies:
        copy.wait()


def on_device(velocity):
    dma, vmem = (pltpu.SemaphoreType.DMA, pltpu.VMEM)
    pencil, level = pl.pallas_call(
        exchange,
        name="exchange",
        out_shape=(vmem((12, 32, 2048), F32), vmem((16, 48, 1024), F32)),
        in_specs=[pl.BlockSpec(memory_space=pl.ANY)],
        out_specs=(pl.BlockSpec(memory_space=vmem), pl.BlockSpec(memory_space=vmem)),
        scratch_shapes=[
            vmem((3, 34, 112, 256), F32),
            vmem((32, 96, 256), F32),
            vmem((96, 32, 256), F32),
            vmem((16, 48, 128), F32),
            vmem((96, 128), F32),
            vmem((4, 48, 128), F32),
            vmem((2, 96, 128), F32),
            vmem((2, 96, 128), F32),
            vmem((2, 2, 32, 2, 128), F32),
            vmem((2, 2, 32, 2, 128), F32),
            vmem((4, 16, 8, 512), F32),
            dma((3, 4)),
            dma((2, 2)),
            dma((2, 2)),
            dma((2, 2)),
            dma((8, 4)),
            dma((8, 4)),
            dma((10, 4)),
            dma((8, 4)),
            dma((4, 4)),
            dma((2, 4)),
        ],
        compiler_params=pltpu.CompilerParams(
            collective_id=0, has_side_effects=True, vmem_limit_bytes=48 * 1024 * 1024
        ),
    )(velocity)
    any_space = pl.BlockSpec(memory_space=pl.ANY)
    local = pl.BlockSpec(memory_space=vmem)
    mag, one, two, three, four, five = pl.pallas_call(
        finish,
        name="finish",
        out_shape=(
            jax.ShapeDtypeStruct((12, 32, 2048), F32),
            jax.ShapeDtypeStruct((16, 48, 1024), F32),
            jax.ShapeDtypeStruct((8, 24, 512), F32),
            jax.ShapeDtypeStruct((12, 4, 256), F32),
            jax.ShapeDtypeStruct((6, 2, 128), F32),
            jax.ShapeDtypeStruct((3, 1, 64), F32),
        ),
        in_specs=[local, local],
        out_specs=(any_space, any_space, local, local, local, local),
        scratch_shapes=[
            vmem((4, 48, 128), F32),
            vmem((24, 128), F32),
            vmem((12, 128), F32),
            vmem((6, 128), F32),
            vmem((4, 12, 256), F32),
            vmem((2, 6, 128), F32),
            dma((2,)),
        ],
        compiler_params=pltpu.CompilerParams(vmem_limit_bytes=16 * 1024 * 1024),
    )(pltpu.with_memory_space_constraint(pencil, vmem), pltpu.with_memory_space_constraint(level, vmem))
    swap = lambda value: jnp.swapaxes(value, 0, 1)
    return swap(mag), one, two, swap(three), swap(four), swap(five)


def solution(mesh):
    in_specs = (P(None, "gx", "gy", "gz"),)
    out_specs = (
        P("gx", ("gy", "gz"), None),
        P("gx", "gy", None),
        P("gx", "gy", None),
        P("gx", "gy", None),
        P("gx", "gy", None),
        P("gx", "gy", None),
    )
    return jax.shard_map(
        on_device, mesh=mesh, in_specs=in_specs, out_specs=out_specs, check_vma=False
    )
```

```python
import functools

import jax
import jax.numpy as jnp
from jax import lax
from jax.experimental import pallas as pl
from jax.experimental.pallas import tpu as pltpu
from jax.sharding import PartitionSpec as P

F32 = jnp.float32
GROUP = 8
ORDER = (1, 2, 0, 3)
U, V, W = (0, 1, 2)


def pairing():
    upper = lax.broadcasted_iota(jnp.int32, (256, 128), 0) // 2
    lower = lax.broadcasted_iota(jnp.int32, (256, 128), 1)
    return (upper == lower).astype(F32)


def lane_pairs(value, pair):
    return jnp.dot(value, pair, precision=lax.Precision.HIGHEST, preferred_element_type=F32)


def lane_pairs_split(value, pair):
    count = value.shape[0]
    high = value.astype(jnp.bfloat16)
    rest = value - high.astype(F32)
    middle = rest.astype(jnp.bfloat16)
    low = (rest - middle.astype(F32)).astype(jnp.bfloat16)
    sums = jnp.dot(
        jnp.concatenate([high, middle, low], axis=0), pair, preferred_element_type=F32
    )
    return sums[0:count] + (sums[count : 2 * count] + sums[2 * count : 3 * count])


def flip(index, mask):
    bits = [(index // w) % 2 for w in (1, 2, 4)]
    bits = [1 - b if (mask >> i) % 2 else b for i, b in enumerate(bits)]
    return bits[0] + 2 * bits[1] + 4 * bits[2]


def exchange(
    vel_hbm, pencil, level, vel, planes, block, own, halves, thirds, edge_out, edge_in, row_out,
    row_in, far, early, patch_out, patch_in, edge_rows, patch_sem, edge_sem, load_sem, x_sem, y_sem, z_sem, a2a_send, a2a_recv, send_sem, level_recv, far_recv,
    own_sem,
):
    gx, gy, gz = (lax.axis_index("gx"), lax.axis_index("gy"), lax.axis_index("gz"))
    half = gz // 4
    FAR, NEAR = ((4, 5, 6, 7), (2, 3, 1, 0))
    far_start, near_start = ((1 - half) * 48, half * 48)
    inside = (gz > 0) & (gz < 7)
    x_sides = [{"gx": (gx + 3) % 4}, {"gx": (gx + 1) % 4}]
    y_sides = [{"gy": (gy + 7) % 8}, {"gy": (gy + 1) % 8}]
    z_sides = [{"gz": (gz + 7) % 8}, {"gz": (gz + 1) % 8}]

    def load(comp, chunk):
        at, planes_in = ((7, 10), (0, 7), (17, 15))[chunk]
        first, count = (0, 96) if comp == V else (8, 80)
        return pltpu.make_async_copy(
            vel_hbm.at[comp, at : at + planes_in, first : first + count],
            vel.at[comp, at + 1 : at + 1 + planes_in, first + 8 : first + 8 + count],
            load_sem.at[comp, chunk],
        )

    def load_side(comp, side):
        return pltpu.make_async_copy(
            vel_hbm.at[comp, :, side * 88 : side * 88 + 8],
            vel.at[comp, 1:33, side * 88 + 8 : side * 88 + 16],
            load_sem.at[3, comp + side],
        )

    sides = [load_side(comp, side) for comp in (U, W) for side in (0, 1)]
    firsts = [load(comp, 0) for comp in (U, V, W)]
    seconds = [load(comp, chunk) for chunk in (1, 2) for comp in (U, V)]
    thirds_in = [load(W, chunk) for chunk in (1, 2)]
    for copy in sides + firsts + seconds + thirds_in:
        copy.start()

    barrier = pltpu.get_barrier_semaphore()
    for mask in range(1, 8):
        pl.semaphore_signal(barrier, inc=1, device_id={"gz": flip(gz, mask)})
    for side in x_sides:
        pl.semaphore_signal(barrier, inc=1, device_id=side)
    opens = [gy >= 4, (gy < 3) | (gy == 7)]
    for side in (0, 1):

        @pl.when(jnp.logical_not(opens[side]))
        def _():
            pl.semaphore_signal(barrier, inc=1, device_id=y_sides[side])

    greeted = 9 + opens[0].astype(jnp.int32) + opens[1].astype(jnp.int32)

    z_halos, y_halos, x_halos = ([], [], [])
    for side in (0, 1):
        z_halos.append(
            pltpu.make_async_remote_copy(
                edge_out.at[side], edge_in.at[1 - side], z_sem.at[0, side], z_sem.at[1, 1 - side],
                device_id=z_sides[side],
            )
        )
        y_halos.append(
            pltpu.make_async_remote_copy(
                row_out.at[side], row_in.at[1 - side], y_sem.at[0, side], y_sem.at[1, 1 - side],
                device_id=y_sides[side],
            )
        )
        x_halos.append(
            pltpu.make_async_remote_copy(
                vel.at[1:3, 31 * side + 1, 8:104], vel.at[1:3, 33 - 33 * side, 8:104],
                x_sem.at[0, side], x_sem.at[1, 1 - side], device_id=x_sides[side],
            )
        )

    def pack_rows(x, carry):
        for spot, comp in enumerate((U, W)):
            for h in (0, 1):
                lanes = slice(h * 128, h * 128 + 128)
                row_out[0, spot, x, h : h + 1, :] = vel[comp, x + 1, 8:9, lanes]
                row_out[1, spot, x, h : h + 1, :] = vel[comp, x + 1, 103:104, lanes]
        return carry

    lane = lax.broadcasted_iota(jnp.int32, (96, 128), 1)

    def pack_edges(x, carry):
        first, last = carry
        for comp in (U, V):
            at = comp * 32 + x
            low, high = (vel[comp, x + 1, 8:104, 0:128], vel[comp, x + 1, 8:104, 128:256])
            first = jnp.where(lane == at, pltpu.roll(low, at, 1), first)
            last = jnp.where(lane == at, pltpu.roll(high, at + 1, 1), last)
        return first, last

    for copy in sides:
        copy.wait()
    lax.fori_loop(0, 32, pack_rows, 0)
    pl.semaphore_wait(barrier, greeted)
    for side in (0, 1):

        @pl.when(opens[side])
        def _():
            y_halos[side].start()

    pair = pairing().astype(jnp.bfloat16)

    def magnitude_rows(x, start, count, edged):
        rows = pl.ds(pl.multiple_of(start, 8), count)
        inner = pl.ds(pl.multiple_of(start + 8, 8), count)
        outer = pl.ds(pl.multiple_of(start, 8), count + 16)
        column = lax.broadcasted_iota(jnp.int32, (count, 128), 1)

        for h in (0, 1):
            lanes = slice(h * 128, h * 128 + 128)

            def second_diff(comp):
                value = vel[comp, x + 1, outer, lanes]
                ahead = pltpu.roll(value, count + 15, 0)
                behind = pltpu.roll(value, 1, 0)
                return (ahead - behind)[8 : 8 + count]

            def third_diff(comp):
                low = vel[comp, x + 1, inner, 0:128]
                high = vel[comp, x + 1, inner, 128:256]
                at = comp * 32 + x
                if h == 0:
                    into_first = pltpu.roll(edge_in[0, rows, :], (128 - at) % 128, 1) if edged else 0.0
                    into_last, here = (pltpu.roll(high, 127, 1), low)
                else:
                    into_last = pltpu.roll(edge_in[1, rows, :], 127 - at, 1) if edged else 0.0
                    into_first, here = (pltpu.roll(low, 1, 1), high)
                ahead = jnp.where(column == 127, into_last, pltpu.roll(here, 127, 1))
                behind = jnp.where(column == 0, into_first, pltpu.roll(here, 1, 1))
                return ahead - behind

            def first_diff(comp):
                return vel[comp, x + 2, inner, lanes] - vel[comp, x, inner, lanes]

            one = second_diff(W) - third_diff(V)
            total = one * one
            two = third_diff(U) - first_diff(W)
            total = total + two * two
            three = first_diff(V) - second_diff(U)
            total = total + three * three
            planes[x, rows, lanes] = jnp.sqrt(1.0 + 0.25 * total)

    def make_rows(part, start, count, edged=True, side=None):
        def one_plane(i, carry):
            magnitude_rows(part * 8 + i, start, count, edged)
            return carry

        lax.fori_loop(0, GROUP, one_plane, 0)

        def turn(y, carry):
            rows = pl.ds(pl.multiple_of(start + y * 8, 8), 8)
            for h in (0, 1):
                lanes = slice(h * 128, h * 128 + 128)
                value = jnp.swapaxes(planes[part * 8 : part * 8 + 8, rows, lanes], 0, 1)
                if side is not None:
                    edge_rows[side, part * 8 : part * 8 + 8, lanes] = value[7 * side]
                elif edged:
                    block[rows, part * 8 : part * 8 + 8, lanes] = value
                else:
                    spot = pl.ds(pl.multiple_of(start - far_start + y * 8, 8), 8)
                    early[spot, :, lanes] = value
            return carry

        lax.fori_loop(0, count // 8, turn, 0)

    def piece_copy(mask, part, edge, first=False):
        target = flip(gz, mask)
        rows = pl.ds(part * 8, 8)
        lanes = pl.ds(pl.multiple_of(gz * 256, 256), 256)
        skip = (target == 0).astype(jnp.int32) if edge else 0
        count = 11 if edge else 12
        source = block.at[pl.ds(target * 12 + skip, count), rows, :]
        if first:
            source = early.at[pl.ds((target % 4) * 12 + skip, count)]
        place = pencil.at[pl.ds(skip, count), rows, lanes]
        if mask == 0:
            return pltpu.make_async_copy(source, place, own_sem.at[1, part])
        return pltpu.make_async_remote_copy(
            source, place, a2a_send.at[mask, part], a2a_recv.at[mask, part],
            device_id={"gz": target},
        )

    def row_copy(mask):
        target = flip(gz, mask)
        high = (target == 7).astype(jnp.int32)
        lanes = pl.ds(pl.multiple_of(gz * 256, 256), 256)
        source = edge_rows.at[pl.ds(high, 1), :, :]
        place = pencil.at[pl.ds(11 * high, 1), :, lanes]
        if mask == 0:
            return pltpu.make_async_copy(source, place, edge_sem.at[0, 0])
        return pltpu.make_async_remote_copy(
            source, place, edge_sem.at[0, mask], edge_sem.at[1, mask], device_id={"gz": target}
        )

    def either(interior, act):
        @pl.when(interior)
        def _():
            act(False)

        @pl.when(jnp.logical_not(interior))
        def _():
            act(True)

    def inner(target):
        return (target > 0) & (target < 7)

    def piece_arrives(mask, part):
        either(inside, lambda edge: piece_copy(mask, part, edge).wait_recv())

    def rows_arrive(masks):
        @pl.when(jnp.logical_not(inside))
        def _():
            for mask in masks:
                row_copy(mask).wait_recv()

    def patch_copy(mask):
        return pltpu.make_async_remote_copy(
            patch_out.at[mask - 4], patch_in.at[mask - 4],
            patch_sem.at[0, mask - 4], patch_sem.at[1, mask - 4], device_id={"gz": flip(gz, mask)},
        )

    column8 = lax.broadcasted_iota(jnp.int32, (8, 128), 1)

    def send_patches():
        for mask in FAR:
            target = flip(gz, mask)
            patch = jnp.zeros((8, 128), F32)
            for r in range(12):
                low = block[target * 12 + r, 8:16, 0:128]
                high = block[target * 12 + r, 8:16, 128:256]
                patch = jnp.where(column8 == 2 * r, pltpu.roll(low, 2 * r, 1), patch)
                patch = jnp.where(column8 == 2 * r + 1, pltpu.roll(high, 2 * r + 2, 1), patch)
            patch_out[mask - 4] = patch
            patch_copy(mask).start()

    def apply_patches():
        for mask in FAR:
            source = flip(gz, mask)
            low = pl.ds(pl.multiple_of(source * 256, 128), 128)
            high = pl.ds(pl.multiple_of(source * 256 + 128, 128), 128)
            patch_copy(mask).wait_recv()
            patch = patch_in[mask - 4]

            def patch_row(r):
                into_low = pltpu.roll(patch, (128 - 2 * r) % 128, 1)
                into_high = pltpu.roll(patch, 126 - 2 * r, 1)
                pencil[r, 8:16, low] = jnp.where(column8 == 0, into_low, pencil[r, 8:16, low])
                pencil[r, 8:16, high] = jnp.where(column8 == 127, into_high, pencil[r, 8:16, high])

            for r in range(1, 11):
                patch_row(r)

            @pl.when(gz > 0)
            def _():
                patch_row(0)

            @pl.when(gz < 7)
            def _():
                patch_row(11)

    def send_pieces(masks, part, first=False):
        for mask in masks:
            either(
                inner(flip(gz, mask)), lambda edge: piece_copy(mask, part, edge, first).start()
            )

    def level_copy(kind, part, origin, target, mine=False):
        every = kind < 3 or part == 3
        first = 0 if every else pl.multiple_of((origin // 4) * 24, 8)
        rows = pl.ds(first, 48 if every else 24)
        parts = pl.ds(part * 4, 4)
        lanes = pl.ds(pl.multiple_of(origin * 128, 128), 128)
        place = level.at[parts, rows, lanes]
        return pltpu.make_async_remote_copy(
            own.at[parts, rows] if mine else place, place,
            send_sem.at[kind, part], level_recv.at[origin, part], device_id={"gz": target},
        )

    def far_copy(kind, part, origin, target):
        place = far.at[origin % 4, pl.ds(part * 4, 4)]
        return pltpu.make_async_remote_copy(
            place, place, send_sem.at[kind, part], far_recv.at[origin % 4, part],
            device_id={"gz": target},
        )

    def own_copy(part):
        lanes = pl.ds(pl.multiple_of(gz * 128, 128), 128)
        return pltpu.make_async_copy(
            own.at[pl.ds(part * 4, 4)], level.at[pl.ds(part * 4, 4), :, lanes], own_sem.at[0, part]
        )

    mate, beside, across, past = (flip(gz, 1), flip(gz, 2), flip(gz, 6), flip(gz, 4))

    for copy in firsts + seconds:
        copy.wait()
    edges = (jnp.zeros((96, 128), F32), jnp.zeros((96, 128), F32))
    edges = lax.fori_loop(0, 32, pack_edges, edges)
    edge_out[0] = edges[0]
    edge_out[1] = edges[1]
    for copy in z_halos:
        copy.start()
    for masks, start in (((4, 5), 24 * ((gz // 2 + 2) % 4)), ((6, 7), 24 * (3 - gz // 2))):
        make_rows(1, start, 24, False)
        send_pieces(masks, 1, True)
    for copy in thirds_in:
        copy.wait()
    for copy in x_halos:
        copy.start()
    for copy in z_halos:
        copy.wait_recv()

    for part in (2, 1, 0, 3):
        if part == 1:
            make_rows(part, far_start, 48)
            send_patches()
        if part == 0:
            for side in (0, 1):

                @pl.when(jnp.logical_not(opens[side]))
                def _():
                    y_halos[1 - side].wait_recv()
                    y_halos[side].start()

            for copy in x_halos:
                copy.wait_recv()
        if part != 1:
            make_rows(part, far_start, 48)
            if part != 3:
                send_pieces(FAR, part)
        make_rows(part, near_start, 48)
        if part != 3:
            send_pieces(NEAR, part)

    for side in (0, 1):

        @pl.when(opens[side])
        def _():
            y_halos[1 - side].wait_recv()


    def fill_rows(x, carry):
        for spot, comp in enumerate((U, W)):
            for h in (0, 1):
                lanes = slice(h * 128, h * 128 + 128)
                vel[comp, x + 1, 7:8, lanes] = row_in[0, spot, x, h : h + 1, :]
                vel[comp, x + 1, 104:105, lanes] = row_in[1, spot, x, h : h + 1, :]
        return carry

    lax.fori_loop(0, 32, fill_rows, 0)
    for part in ORDER:
        make_rows(part, 0, 8, side=0)
        make_rows(part, 88, 8, side=1)
        summed = [planes[2 * j] + planes[2 * j + 1] for j in range(part * 4, part * 4 + 4)]
        halves[...] = lane_pairs_split(jnp.concatenate(summed, axis=0), pair)
        for j in range(4):
            even = halves[pl.ds(j * 96, 48, stride=2), :]
            odd = halves[pl.ds(j * 96 + 1, 48, stride=2), :]
            own[part * 4 + j] = (even + odd) * 0.125
        level_copy(3, part, gz, across, True).start()
        level_copy(1, part, gz, beside, True).start()
        level_copy(0, part, gz, mate, True).start()
        own_copy(part).start()
    for mask in FAR + NEAR:

        @pl.when(jnp.logical_not(inner(flip(gz, mask))))
        def _():
            row_copy(mask).start()

    send_pieces(FAR[:2] + NEAR, 3)

    def pass_far(part):
        for mask in FAR:
            piece_arrives(mask, part)
        if part == 1:
            apply_patches()
            rows_arrive(FAR)
        parts = pl.ds(part * 8, 8)
        rows = []
        for s in range(4):
            lanes = pl.ds(pl.multiple_of((1 - half) * 1024 + s * 256, 256), 256)
            rows += [pencil[2 * r, parts, lanes] + pencil[2 * r + 1, parts, lanes] for r in range(6)]
        pooled = lane_pairs_split(jnp.concatenate(rows, axis=0), pair)
        for s in range(4):
            thirds[s] = pooled[s * 48 : s * 48 + 48]
            for j in range(4):
                even = thirds[s, pl.ds(2 * j, 6, stride=8), :]
                odd = thirds[s, pl.ds(2 * j + 1, 6, stride=8), :]
                far[gz % 4, part * 4 + j, 0:6, s * 128 : s * 128 + 128] = (even + odd) * 0.125
        far_copy(8, part, gz, beside).start()
        far_copy(7, part, gz, mate).start()

    def pass_level(part):
        level_copy(3, part, across, across).wait_recv()
        level_copy(4, part, across, beside).start()
        level_copy(5, part, across, mate).start()

    for part in ORDER:
        level_copy(1, part, beside, beside).wait_recv()
        level_copy(2, part, beside, mate).start()
    pass_far(1)
    send_pieces(FAR[2:], 3)
    pass_far(2)
    pass_far(0)
    for part in ORDER:
        pass_level(part)
    for part in ORDER[:3]:
        far_copy(8, part, beside, beside).wait_recv()
        far_copy(9, part, beside, mate).start()
    for part in ORDER:
        level_copy(4, part, past, beside).wait_recv()
        level_copy(6, part, past, mate).start()

    for part in ORDER:
        own_copy(part).wait()
        level_copy(0, part, mate, mate).wait_recv()
        level_copy(2, part, flip(gz, 3), mate).wait_recv()
        level_copy(5, part, flip(gz, 7), mate).wait_recv()
        level_copy(6, part, flip(gz, 5), mate).wait_recv()
        if part != 3:
            far_copy(7, part, mate, mate).wait_recv()
            far_copy(9, part, flip(gz, 3), mate).wait_recv()

    for side in (0, 1):

        @pl.when(half == side)
        def _():
            for d in range(4):
                rows = slice(side * 24 + d * 6, side * 24 + d * 6 + 6)
                lanes = slice((1 - side) * 512, (1 - side) * 512 + 512)

                def place_rows(j, carry):
                    level[j, rows, lanes] = far[d, j, 0:6, :]
                    return carry

                lax.fori_loop(0, 12, place_rows, 0)

    for part in ORDER:
        level_copy(0, part, gz, mate).wait_send()
        level_copy(1, part, gz, beside).wait_send()
        level_copy(2, part, beside, mate).wait_send()
        level_copy(3, part, gz, across).wait_send()
        level_copy(4, part, across, beside).wait_send()
        level_copy(5, part, across, mate).wait_send()
        level_copy(6, part, past, mate).wait_send()
        if part != 3:
            far_copy(7, part, gz, mate).wait_send()
            far_copy(8, part, gz, beside).wait_send()
            far_copy(9, part, beside, mate).wait_send()
    for copy in z_halos + y_halos + x_halos:
        copy.wait_send()
    for mask in FAR:
        patch_copy(mask).wait_send()
    for mask in range(1, 8):

        @pl.when(jnp.logical_not(inner(flip(gz, mask))))
        def _():
            row_copy(mask).wait_send()

    rows_arrive((1, 2, 3))

    @pl.when(jnp.logical_not(inside))
    def _():
        row_copy(0).wait()

    for part in ORDER:
        either(inside, lambda edge: piece_copy(0, part, edge).wait())
        for mask in range(1, 8):
            either(inner(flip(gz, mask)), lambda edge: piece_copy(mask, part, edge).wait_send())
        for mask in (1, 2, 3) + (FAR if part == 3 else ()):
            piece_arrives(mask, part)


def finish(
    pencil, level, mag_out, one_out, two_out, three_out, four_out, five_out,
    two_half, three_half, four_half, five_half, three_at, four_at, sems,
):
    copies = [
        pltpu.make_async_copy(pencil.at[i * 3 : i * 3 + 3], mag_out.at[i * 3 : i * 3 + 3], sems.at[0, i])
        for i in range(4)
    ] + [
        pltpu.make_async_copy(level.at[i * 4 : i * 4 + 4], one_out.at[i * 4 : i * 4 + 4], sems.at[1, i])
        for i in range(4)
    ]
    for copy in copies:
        copy.start()
    pair = pairing()

    def step(low, high, half, rows, lanes):
        summed = low + high
        if lanes >= 256:
            for s in range(lanes // 256):
                half[0:rows, s * 128 : s * 128 + 128] = lane_pairs(
                    summed[:, s * 256 : s * 256 + 256], pair
                )
        else:
            half[0:rows, 0:64] = lane_pairs(summed, pair[0:128, 0:64])
        width = lanes // 2
        even = half[pl.ds(0, rows // 2, stride=2), 0:width]
        odd = half[pl.ds(1, rows // 2, stride=2), 0:width]
        return (even + odd) * 0.125

    for i in range(8):
        for s in range(4):
            summed = level[2 * i, :, s * 256 : s * 256 + 256] + level[2 * i + 1, :, s * 256 : s * 256 + 256]
            two_half[s, :, :] = lane_pairs(summed, pair)
            even = two_half[s, pl.ds(0, 24, stride=2), :]
            odd = two_half[s, pl.ds(1, 24, stride=2), :]
            two_out[i, :, s * 128 : s * 128 + 128] = (even + odd) * 0.125
    for i in range(4):
        for s in range(2):
            lanes = slice(s * 256, s * 256 + 256)
            three_half[...] = lane_pairs(two_out[2 * i, :, lanes] + two_out[2 * i + 1, :, lanes], pair)
            even = three_half[pl.ds(0, 12, stride=2), :]
            odd = three_half[pl.ds(1, 12, stride=2), :]
            value = (even + odd) * 0.125
            three_at[i, :, s * 128 : s * 128 + 128] = value
            for r in range(12):
                three_out[r, i : i + 1, s * 128 : s * 128 + 128] = value[r : r + 1]
    for i in range(2):
        four_half[...] = lane_pairs(three_at[2 * i] + three_at[2 * i + 1], pair)
        value = (four_half[pl.ds(0, 6, stride=2), :] + four_half[pl.ds(1, 6, stride=2), :]) * 0.125
        four_at[i] = value
        for r in range(6):
            four_out[r, i : i + 1, :] = value[r : r + 1]
    five_half[...] = lane_pairs(four_at[0] + four_at[1], pair[0:128, :])
    value = (five_half[pl.ds(0, 3, stride=2), :] + five_half[pl.ds(1, 3, stride=2), :]) * 0.125
    for r in range(3):
        five_out[r] = value[r : r + 1, 0:64]
    for copy in copies:
        copy.wait()


def on_device(velocity):
    dma, vmem = (pltpu.SemaphoreType.DMA, pltpu.VMEM)
    pencil, level = pl.pallas_call(
        exchange,
        name="exchange",
        out_shape=(vmem((12, 32, 2048), F32), vmem((16, 48, 1024), F32)),
        in_specs=[pl.BlockSpec(memory_space=pl.ANY)],
        out_specs=(pl.BlockSpec(memory_space=vmem), pl.BlockSpec(memory_space=vmem)),
        scratch_shapes=[
            vmem((3, 34, 112, 256), F32),
            vmem((32, 96, 256), F32),
            vmem((96, 32, 256), F32),
            vmem((16, 48, 128), F32),
            vmem((384, 128), F32),
            vmem((4, 48, 128), F32),
            vmem((2, 96, 128), F32),
            vmem((2, 96, 128), F32),
            vmem((2, 2, 32, 2, 128), F32),
            vmem((2, 2, 32, 2, 128), F32),
            vmem((4, 12, 8, 512), F32),
            vmem((48, 8, 256), F32),
            vmem((4, 8, 128), F32),
            vmem((4, 8, 128), F32),
            vmem((2, 32, 256), F32),
            dma((2, 4)),
            dma((2, 8)),
            dma((4, 4)),
            dma((2, 2)),
            dma((2, 2)),
            dma((2, 2)),
            dma((8, 4)),
            dma((8, 4)),
            dma((10, 4)),
            dma((8, 4)),
            dma((4, 3)),
            dma((2, 4)),
        ],
        compiler_params=pltpu.CompilerParams(
            collective_id=0, has_side_effects=True, vmem_limit_bytes=48 * 1024 * 1024
        ),
    )(velocity)
    any_space = pl.BlockSpec(memory_space=pl.ANY)
    local = pl.BlockSpec(memory_space=vmem)
    mag, one, two, three, four, five = pl.pallas_call(
        finish,
        name="finish",
        out_shape=(
            jax.ShapeDtypeStruct((12, 32, 2048), F32),
            jax.ShapeDtypeStruct((16, 48, 1024), F32),
            jax.ShapeDtypeStruct((8, 24, 512), F32),
            jax.ShapeDtypeStruct((12, 4, 256), F32),
            jax.ShapeDtypeStruct((6, 2, 128), F32),
            jax.ShapeDtypeStruct((3, 1, 64), F32),
        ),
        in_specs=[local, local],
        out_specs=(any_space, any_space, local, local, local, local),
        scratch_shapes=[
            vmem((4, 48, 128), F32),
            vmem((24, 128), F32),
            vmem((12, 128), F32),
            vmem((6, 128), F32),
            vmem((4, 12, 256), F32),
            vmem((2, 6, 128), F32),
            dma((2, 4)),
        ],
        compiler_params=pltpu.CompilerParams(vmem_limit_bytes=16 * 1024 * 1024),
    )(pltpu.with_memory_space_constraint(pencil, vmem), pltpu.with_memory_space_constraint(level, vmem))
    swap = lambda value: jnp.swapaxes(value, 0, 1)
    return swap(mag), one, two, swap(three), swap(four), swap(five)


def solution(mesh):
    in_specs = (P(None, "gx", "gy", "gz"),)
    out_specs = (
        P("gx", ("gy", "gz"), None),
        P("gx", "gy", None),
        P("gx", "gy", None),
        P("gx", "gy", None),
        P("gx", "gy", None),
        P("gx", "gy", None),
    )
    return jax.shard_map(
        on_device, mesh=mesh, in_specs=in_specs, out_specs=out_specs, check_vma=False
    )
```

```python
import functools

import jax
import jax.numpy as jnp
from jax import lax
from jax.experimental import pallas as pl
from jax.experimental.pallas import tpu as pltpu
from jax.sharding import PartitionSpec as P

F32 = jnp.float32
GROUP = 8
ORDER = (1, 2, 0, 3)
U, V, W = (0, 1, 2)


def pairing():
    upper = lax.broadcasted_iota(jnp.int32, (256, 128), 0) // 2
    lower = lax.broadcasted_iota(jnp.int32, (256, 128), 1)
    return (upper == lower).astype(F32)


def lane_pairs(value, pair):
    return jnp.dot(value, pair, precision=lax.Precision.HIGHEST, preferred_element_type=F32)


def lane_pairs_split(value, pair):
    count = value.shape[0]
    high = value.astype(jnp.bfloat16)
    rest = value - high.astype(F32)
    middle = rest.astype(jnp.bfloat16)
    low = (rest - middle.astype(F32)).astype(jnp.bfloat16)
    sums = jnp.dot(
        jnp.concatenate([high, middle, low], axis=0), pair, preferred_element_type=F32
    )
    return sums[0:count] + (sums[count : 2 * count] + sums[2 * count : 3 * count])


def flip(index, mask):
    bits = [(index // w) % 2 for w in (1, 2, 4)]
    bits = [1 - b if (mask >> i) % 2 else b for i, b in enumerate(bits)]
    return bits[0] + 2 * bits[1] + 4 * bits[2]


def exchange(
    vel_hbm, pencil, level, vel, planes, block, own, halves, thirds, edge_out, edge_in, row_out,
    row_in, far, early, patch_out, patch_in, edge_rows, patch_sem, edge_sem, load_sem, x_sem, y_sem, z_sem, a2a_send, a2a_recv, send_sem, level_recv, far_recv,
    own_sem,
):
    gx, gy, gz = (lax.axis_index("gx"), lax.axis_index("gy"), lax.axis_index("gz"))
    half = gz // 4
    FAR, NEAR = ((4, 5, 6, 7), (2, 3, 1, 0))
    far_start, near_start = ((1 - half) * 48, half * 48)
    inside = (gz > 0) & (gz < 7)
    x_sides = [{"gx": (gx + 3) % 4}, {"gx": (gx + 1) % 4}]
    y_sides = [{"gy": (gy + 7) % 8}, {"gy": (gy + 1) % 8}]
    z_sides = [{"gz": (gz + 7) % 8}, {"gz": (gz + 1) % 8}]

    def load(comp, chunk):
        at, planes_in = ((7, 10), (0, 7), (17, 15))[chunk]
        first, count = (0, 96) if comp == V else (8, 80)
        return pltpu.make_async_copy(
            vel_hbm.at[comp, at : at + planes_in, first : first + count],
            vel.at[comp, at + 1 : at + 1 + planes_in, first + 8 : first + 8 + count],
            load_sem.at[comp, chunk],
        )

    def load_side(comp, side):
        return pltpu.make_async_copy(
            vel_hbm.at[comp, :, side * 88 : side * 88 + 8],
            vel.at[comp, 1:33, side * 88 + 8 : side * 88 + 16],
            load_sem.at[3, comp + side],
        )

    sides = [load_side(comp, side) for comp in (U, W) for side in (0, 1)]
    firsts = [load(comp, 0) for comp in (U, V, W)]
    seconds = [load(comp, chunk) for chunk in (1, 2) for comp in (U, V)]
    thirds_in = [load(W, chunk) for chunk in (1, 2)]
    for copy in sides + firsts + seconds + thirds_in:
        copy.start()

    barrier = pltpu.get_barrier_semaphore()
    for mask in range(1, 8):
        pl.semaphore_signal(barrier, inc=1, device_id={"gz": flip(gz, mask)})
    for side in x_sides:
        pl.semaphore_signal(barrier, inc=1, device_id=side)
    opens = [gy >= 4, (gy < 3) | (gy == 7)]
    for side in (0, 1):

        @pl.when(jnp.logical_not(opens[side]))
        def _():
            pl.semaphore_signal(barrier, inc=1, device_id=y_sides[side])

    greeted = 9 + opens[0].astype(jnp.int32) + opens[1].astype(jnp.int32)

    z_halos, y_halos, x_halos = ([], [], [])
    for side in (0, 1):
        z_halos.append(
            pltpu.make_async_remote_copy(
                edge_out.at[side], edge_in.at[1 - side], z_sem.at[0, side], z_sem.at[1, 1 - side],
                device_id=z_sides[side],
            )
        )
        y_halos.append(
            pltpu.make_async_remote_copy(
                row_out.at[side], row_in.at[1 - side], y_sem.at[0, side], y_sem.at[1, 1 - side],
                device_id=y_sides[side],
            )
        )
        x_halos.append(
            pltpu.make_async_remote_copy(
                vel.at[1:3, 31 * side + 1, 8:104], vel.at[1:3, 33 - 33 * side, 8:104],
                x_sem.at[0, side], x_sem.at[1, 1 - side], device_id=x_sides[side],
            )
        )

    def pack_rows(x, carry):
        for spot, comp in enumerate((U, W)):
            for h in (0, 1):
                lanes = slice(h * 128, h * 128 + 128)
                row_out[0, spot, x, h : h + 1, :] = vel[comp, x + 1, 8:9, lanes]
                row_out[1, spot, x, h : h + 1, :] = vel[comp, x + 1, 103:104, lanes]
        return carry

    lane = lax.broadcasted_iota(jnp.int32, (96, 128), 1)

    def pack_edges(x, carry):
        first, last = carry
        for comp in (U, V):
            at = comp * 32 + x
            low, high = (vel[comp, x + 1, 8:104, 0:128], vel[comp, x + 1, 8:104, 128:256])
            first = jnp.where(lane == at, pltpu.roll(low, at, 1), first)
            last = jnp.where(lane == at, pltpu.roll(high, at + 1, 1), last)
        return first, last

    for copy in sides:
        copy.wait()
    lax.fori_loop(0, 32, pack_rows, 0)
    pl.semaphore_wait(barrier, greeted)
    for side in (0, 1):

        @pl.when(opens[side])
        def _():
            y_halos[side].start()

    pair = pairing().astype(jnp.bfloat16)

    def magnitude_rows(x, start, count, edged):
        rows = pl.ds(pl.multiple_of(start, 8), count)
        inner = pl.ds(pl.multiple_of(start + 8, 8), count)
        outer = pl.ds(pl.multiple_of(start, 8), count + 16)
        column = lax.broadcasted_iota(jnp.int32, (count, 128), 1)

        for h in (0, 1):
            lanes = slice(h * 128, h * 128 + 128)

            def second_diff(comp):
                value = vel[comp, x + 1, outer, lanes]
                ahead = pltpu.roll(value, count + 15, 0)
                behind = pltpu.roll(value, 1, 0)
                return (ahead - behind)[8 : 8 + count]

            def third_diff(comp):
                low = vel[comp, x + 1, inner, 0:128]
                high = vel[comp, x + 1, inner, 128:256]
                at = comp * 32 + x
                if h == 0:
                    into_first = pltpu.roll(edge_in[0, rows, :], (128 - at) % 128, 1) if edged else 0.0
                    into_last, here = (pltpu.roll(high, 127, 1), low)
                else:
                    into_last = pltpu.roll(edge_in[1, rows, :], 127 - at, 1) if edged else 0.0
                    into_first, here = (pltpu.roll(low, 1, 1), high)
                ahead = jnp.where(column == 127, into_last, pltpu.roll(here, 127, 1))
                behind = jnp.where(column == 0, into_first, pltpu.roll(here, 1, 1))
                return ahead - behind

            def first_diff(comp):
                return vel[comp, x + 2, inner, lanes] - vel[comp, x, inner, lanes]

            one = second_diff(W) - third_diff(V)
            total = one * one
            two = third_diff(U) - first_diff(W)
            total = total + two * two
            three = first_diff(V) - second_diff(U)
            total = total + three * three
            planes[x, rows, lanes] = jnp.sqrt(1.0 + 0.25 * total)

    def make_rows(part, start, count, edged=True, side=None):
        def one_plane(i, carry):
            magnitude_rows(part * 8 + i, start, count, edged)
            return carry

        lax.fori_loop(0, GROUP, one_plane, 0)

        def turn(y, carry):
            rows = pl.ds(pl.multiple_of(start + y * 8, 8), 8)
            for h in (0, 1):
                lanes = slice(h * 128, h * 128 + 128)
                value = jnp.swapaxes(planes[part * 8 : part * 8 + 8, rows, lanes], 0, 1)
                if side is not None:
                    edge_rows[side, part * 8 : part * 8 + 8, lanes] = value[7 * side]
                elif edged:
                    block[rows, part * 8 : part * 8 + 8, lanes] = value
                else:
                    spot = pl.ds(pl.multiple_of(start - far_start + y * 8, 8), 8)
                    early[spot, :, lanes] = value
            return carry

        lax.fori_loop(0, count // 8, turn, 0)

    def piece_copy(mask, part, edge, first=False):
        target = flip(gz, mask)
        rows = pl.ds(part * 8, 8)
        lanes = pl.ds(pl.multiple_of(gz * 256, 256), 256)
        skip = (target == 0).astype(jnp.int32) if edge else 0
        count = 11 if edge else 12
        source = block.at[pl.ds(target * 12 + skip, count), rows, :]
        if first:
            source = early.at[pl.ds((target % 4) * 12 + skip, count)]
        place = pencil.at[pl.ds(skip, count), rows, lanes]
        if mask == 0:
            return pltpu.make_async_copy(source, place, own_sem.at[1, part])
        return pltpu.make_async_remote_copy(
            source, place, a2a_send.at[mask, part], a2a_recv.at[mask, part],
            device_id={"gz": target},
        )

    def row_copy(mask):
        target = flip(gz, mask)
        high = (target == 7).astype(jnp.int32)
        lanes = pl.ds(pl.multiple_of(gz * 256, 256), 256)
        source = edge_rows.at[pl.ds(high, 1), :, :]
        place = pencil.at[pl.ds(11 * high, 1), :, lanes]
        if mask == 0:
            return pltpu.make_async_copy(source, place, edge_sem.at[0, 0])
        return pltpu.make_async_remote_copy(
            source, place, edge_sem.at[0, mask], edge_sem.at[1, mask], device_id={"gz": target}
        )

    def either(interior, act):
        @pl.when(interior)
        def _():
            act(False)

        @pl.when(jnp.logical_not(interior))
        def _():
            act(True)

    def inner(target):
        return (target > 0) & (target < 7)

    def piece_arrives(mask, part):
        either(inside, lambda edge: piece_copy(mask, part, edge).wait_recv())

    def rows_arrive(masks):
        @pl.when(jnp.logical_not(inside))
        def _():
            for mask in masks:
                row_copy(mask).wait_recv()

    def patch_copy(mask):
        return pltpu.make_async_remote_copy(
            patch_out.at[mask - 4], patch_in.at[mask - 4],
            patch_sem.at[0, mask - 4], patch_sem.at[1, mask - 4], device_id={"gz": flip(gz, mask)},
        )

    column8 = lax.broadcasted_iota(jnp.int32, (8, 128), 1)

    def send_patches():
        for mask in FAR:
            target = flip(gz, mask)
            patch = jnp.zeros((8, 128), F32)
            for r in range(12):
                low = block[target * 12 + r, 8:16, 0:128]
                high = block[target * 12 + r, 8:16, 128:256]
                patch = jnp.where(column8 == 2 * r, pltpu.roll(low, 2 * r, 1), patch)
                patch = jnp.where(column8 == 2 * r + 1, pltpu.roll(high, 2 * r + 2, 1), patch)
            patch_out[mask - 4] = patch
            patch_copy(mask).start()

    def apply_patches():
        for mask in FAR:
            source = flip(gz, mask)
            low = pl.ds(pl.multiple_of(source * 256, 128), 128)
            high = pl.ds(pl.multiple_of(source * 256 + 128, 128), 128)
            patch_copy(mask).wait_recv()
            patch = patch_in[mask - 4]

            def patch_row(r):
                into_low = pltpu.roll(patch, (128 - 2 * r) % 128, 1)
                into_high = pltpu.roll(patch, 126 - 2 * r, 1)
                pencil[r, 8:16, low] = jnp.where(column8 == 0, into_low, pencil[r, 8:16, low])
                pencil[r, 8:16, high] = jnp.where(column8 == 127, into_high, pencil[r, 8:16, high])

            for r in range(1, 11):
                patch_row(r)

            @pl.when(gz > 0)
            def _():
                patch_row(0)

            @pl.when(gz < 7)
            def _():
                patch_row(11)

    def send_pieces(masks, part, first=False):
        for mask in masks:
            either(
                inner(flip(gz, mask)), lambda edge: piece_copy(mask, part, edge, first).start()
            )

    def level_copy(kind, part, origin, target, mine=False):
        every = kind < 3 or part == 3
        first = 0 if every else pl.multiple_of((origin // 4) * 24, 8)
        rows = pl.ds(first, 48 if every else 24)
        parts = pl.ds(part * 4, 4)
        lanes = pl.ds(pl.multiple_of(origin * 128, 128), 128)
        place = level.at[parts, rows, lanes]
        return pltpu.make_async_remote_copy(
            own.at[parts, rows] if mine else place, place,
            send_sem.at[kind, part], level_recv.at[origin, part], device_id={"gz": target},
        )

    def far_copy(kind, part, origin, target):
        place = far.at[origin % 4, pl.ds(part * 4, 4)]
        return pltpu.make_async_remote_copy(
            place, place, send_sem.at[kind, part], far_recv.at[origin % 4, part],
            device_id={"gz": target},
        )

    def own_copy(part):
        lanes = pl.ds(pl.multiple_of(gz * 128, 128), 128)
        return pltpu.make_async_copy(
            own.at[pl.ds(part * 4, 4)], level.at[pl.ds(part * 4, 4), :, lanes], own_sem.at[0, part]
        )

    mate, beside, across, past = (flip(gz, 1), flip(gz, 2), flip(gz, 6), flip(gz, 4))

    for copy in firsts + seconds:
        copy.wait()
    edges = (jnp.zeros((96, 128), F32), jnp.zeros((96, 128), F32))
    edges = lax.fori_loop(0, 32, pack_edges, edges)
    edge_out[0] = edges[0]
    edge_out[1] = edges[1]
    for copy in z_halos:
        copy.start()
    for masks, start in (((4, 5), 24 * ((gz // 2 + 2) % 4)), ((6, 7), 24 * (3 - gz // 2))):
        make_rows(1, start, 24, False)
        send_pieces(masks, 1, True)
    for copy in thirds_in:
        copy.wait()
    for copy in x_halos:
        copy.start()
    for copy in z_halos:
        copy.wait_recv()

    for part in (2, 1, 0, 3):
        if part == 1:
            make_rows(part, far_start, 48)
            send_patches()
        if part == 0:
            for side in (0, 1):

                @pl.when(jnp.logical_not(opens[side]))
                def _():
                    y_halos[1 - side].wait_recv()
                    y_halos[side].start()

            for copy in x_halos:
                copy.wait_recv()
        if part != 1:
            make_rows(part, far_start, 48)
            if part != 3:
                send_pieces(FAR, part)
        make_rows(part, near_start, 48)
        if part != 3:
            send_pieces(NEAR, part)

    for side in (0, 1):

        @pl.when(opens[side])
        def _():
            y_halos[1 - side].wait_recv()


    def fill_rows(x, carry):
        for spot, comp in enumerate((U, W)):
            for h in (0, 1):
                lanes = slice(h * 128, h * 128 + 128)
                vel[comp, x + 1, 7:8, lanes] = row_in[0, spot, x, h : h + 1, :]
                vel[comp, x + 1, 104:105, lanes] = row_in[1, spot, x, h : h + 1, :]
        return carry

    lax.fori_loop(0, 32, fill_rows, 0)
    for part in ORDER:
        make_rows(part, 0, 8, side=0)
        make_rows(part, 88, 8, side=1)
        summed = [planes[2 * j] + planes[2 * j + 1] for j in range(part * 4, part * 4 + 4)]
        halves[...] = lane_pairs_split(jnp.concatenate(summed, axis=0), pair)
        for j in range(4):
            even = halves[pl.ds(j * 96, 48, stride=2), :]
            odd = halves[pl.ds(j * 96 + 1, 48, stride=2), :]
            own[part * 4 + j] = (even + odd) * 0.125
        level_copy(1, part, gz, beside, True).start()
        level_copy(0, part, gz, mate, True).start()
        level_copy(3, part, gz, across, True).start()
        own_copy(part).start()
    for mask in FAR + NEAR:

        @pl.when(jnp.logical_not(inner(flip(gz, mask))))
        def _():
            row_copy(mask).start()

    send_pieces(FAR[:2] + NEAR, 3)

    def pass_far(part):
        for mask in FAR:
            piece_arrives(mask, part)
        if part == 1:
            apply_patches()
            rows_arrive(FAR)
        parts = pl.ds(part * 8, 8)
        rows = []
        for s in range(4):
            lanes = pl.ds(pl.multiple_of((1 - half) * 1024 + s * 256, 256), 256)
            rows += [pencil[2 * r, parts, lanes] + pencil[2 * r + 1, parts, lanes] for r in range(6)]
        pooled = lane_pairs_split(jnp.concatenate(rows, axis=0), pair)
        for s in range(4):
            thirds[s] = pooled[s * 48 : s * 48 + 48]
            for j in range(4):
                even = thirds[s, pl.ds(2 * j, 6, stride=8), :]
                odd = thirds[s, pl.ds(2 * j + 1, 6, stride=8), :]
                far[gz % 4, part * 4 + j, 0:6, s * 128 : s * 128 + 128] = (even + odd) * 0.125
        far_copy(8, part, gz, beside).start()
        far_copy(7, part, gz, mate).start()

    def pass_level(part):
        level_copy(3, part, across, across).wait_recv()
        level_copy(4, part, across, beside).start()
        level_copy(5, part, across, mate).start()

    for part in ORDER:
        level_copy(1, part, beside, beside).wait_recv()
        level_copy(2, part, beside, mate).start()
    pass_far(1)
    send_pieces(FAR[2:], 3)
    pass_far(2)
    pass_far(0)
    for part in ORDER:
        pass_level(part)
    for part in ORDER[:3]:
        far_copy(8, part, beside, beside).wait_recv()
        far_copy(9, part, beside, mate).start()
    for part in ORDER:
        level_copy(4, part, past, beside).wait_recv()
        level_copy(6, part, past, mate).start()

    for part in ORDER:
        own_copy(part).wait()
        level_copy(0, part, mate, mate).wait_recv()
        level_copy(2, part, flip(gz, 3), mate).wait_recv()
        level_copy(5, part, flip(gz, 7), mate).wait_recv()
        level_copy(6, part, flip(gz, 5), mate).wait_recv()
        if part != 3:
            far_copy(7, part, mate, mate).wait_recv()
            far_copy(9, part, flip(gz, 3), mate).wait_recv()

    for side in (0, 1):

        @pl.when(half == side)
        def _():
            for d in range(4):
                rows = slice(side * 24 + d * 6, side * 24 + d * 6 + 6)
                lanes = slice((1 - side) * 512, (1 - side) * 512 + 512)

                def place_rows(j, carry):
                    level[j, rows, lanes] = far[d, j, 0:6, :]
                    return carry

                lax.fori_loop(0, 12, place_rows, 0)

    for part in ORDER:
        level_copy(0, part, gz, mate).wait_send()
        level_copy(1, part, gz, beside).wait_send()
        level_copy(2, part, beside, mate).wait_send()
        level_copy(3, part, gz, across).wait_send()
        level_copy(4, part, across, beside).wait_send()
        level_copy(5, part, across, mate).wait_send()
        level_copy(6, part, past, mate).wait_send()
        if part != 3:
            far_copy(7, part, gz, mate).wait_send()
            far_copy(8, part, gz, beside).wait_send()
            far_copy(9, part, beside, mate).wait_send()
    for copy in z_halos + y_halos + x_halos:
        copy.wait_send()
    for mask in FAR:
        patch_copy(mask).wait_send()
    for mask in range(1, 8):

        @pl.when(jnp.logical_not(inner(flip(gz, mask))))
        def _():
            row_copy(mask).wait_send()

    rows_arrive((1, 2, 3))

    @pl.when(jnp.logical_not(inside))
    def _():
        row_copy(0).wait()

    for part in ORDER:
        either(inside, lambda edge: piece_copy(0, part, edge).wait())
        for mask in range(1, 8):
            either(inner(flip(gz, mask)), lambda edge: piece_copy(mask, part, edge).wait_send())
        for mask in (1, 2, 3) + (FAR if part == 3 else ()):
            piece_arrives(mask, part)


def finish(
    pencil, level, mag_out, one_out, two_out, three_out, four_out, five_out,
    two_half, three_half, four_half, five_half, three_at, four_at, sems,
):
    copies = [
        pltpu.make_async_copy(pencil.at[i * 3 : i * 3 + 3], mag_out.at[i * 3 : i * 3 + 3], sems.at[0, i])
        for i in range(4)
    ] + [
        pltpu.make_async_copy(level.at[i * 4 : i * 4 + 4], one_out.at[i * 4 : i * 4 + 4], sems.at[1, i])
        for i in range(4)
    ]
    for copy in copies:
        copy.start()
    pair = pairing()

    def step(low, high, half, rows, lanes):
        summed = low + high
        if lanes >= 256:
            for s in range(lanes // 256):
                half[0:rows, s * 128 : s * 128 + 128] = lane_pairs(
                    summed[:, s * 256 : s * 256 + 256], pair
                )
        else:
            half[0:rows, 0:64] = lane_pairs(summed, pair[0:128, 0:64])
        width = lanes // 2
        even = half[pl.ds(0, rows // 2, stride=2), 0:width]
        odd = half[pl.ds(1, rows // 2, stride=2), 0:width]
        return (even + odd) * 0.125

    for i in range(8):
        for s in range(4):
            summed = level[2 * i, :, s * 256 : s * 256 + 256] + level[2 * i + 1, :, s * 256 : s * 256 + 256]
            two_half[s, :, :] = lane_pairs(summed, pair)
            even = two_half[s, pl.ds(0, 24, stride=2), :]
            odd = two_half[s, pl.ds(1, 24, stride=2), :]
            two_out[i, :, s * 128 : s * 128 + 128] = (even + odd) * 0.125
    for i in range(4):
        for s in range(2):
            lanes = slice(s * 256, s * 256 + 256)
            three_half[...] = lane_pairs(two_out[2 * i, :, lanes] + two_out[2 * i + 1, :, lanes], pair)
            even = three_half[pl.ds(0, 12, stride=2), :]
            odd = three_half[pl.ds(1, 12, stride=2), :]
            value = (even + odd) * 0.125
            three_at[i, :, s * 128 : s * 128 + 128] = value
            for r in range(12):
                three_out[r, i : i + 1, s * 128 : s * 128 + 128] = value[r : r + 1]
    for i in range(2):
        four_half[...] = lane_pairs(three_at[2 * i] + three_at[2 * i + 1], pair)
        value = (four_half[pl.ds(0, 6, stride=2), :] + four_half[pl.ds(1, 6, stride=2), :]) * 0.125
        four_at[i] = value
        for r in range(6):
            four_out[r, i : i + 1, :] = value[r : r + 1]
    five_half[...] = lane_pairs(four_at[0] + four_at[1], pair[0:128, :])
    value = (five_half[pl.ds(0, 3, stride=2), :] + five_half[pl.ds(1, 3, stride=2), :]) * 0.125
    for r in range(3):
        five_out[r] = value[r : r + 1, 0:64]
    for copy in copies:
        copy.wait()


def on_device(velocity):
    dma, vmem = (pltpu.SemaphoreType.DMA, pltpu.VMEM)
    pencil, level = pl.pallas_call(
        exchange,
        name="exchange",
        out_shape=(vmem((12, 32, 2048), F32), vmem((16, 48, 1024), F32)),
        in_specs=[pl.BlockSpec(memory_space=pl.ANY)],
        out_specs=(pl.BlockSpec(memory_space=vmem), pl.BlockSpec(memory_space=vmem)),
        scratch_shapes=[
            vmem((3, 34, 112, 256), F32),
            vmem((32, 96, 256), F32),
            vmem((96, 32, 256), F32),
            vmem((16, 48, 128), F32),
            vmem((384, 128), F32),
            vmem((4, 48, 128), F32),
            vmem((2, 96, 128), F32),
            vmem((2, 96, 128), F32),
            vmem((2, 2, 32, 2, 128), F32),
            vmem((2, 2, 32, 2, 128), F32),
            vmem((4, 12, 8, 512), F32),
            vmem((48, 8, 256), F32),
            vmem((4, 8, 128), F32),
            vmem((4, 8, 128), F32),
            vmem((2, 32, 256), F32),
            dma((2, 4)),
            dma((2, 8)),
            dma((4, 4)),
            dma((2, 2)),
            dma((2, 2)),
            dma((2, 2)),
            dma((8, 4)),
            dma((8, 4)),
            dma((10, 4)),
            dma((8, 4)),
            dma((4, 3)),
            dma((2, 4)),
        ],
        compiler_params=pltpu.CompilerParams(
            collective_id=0, has_side_effects=True, vmem_limit_bytes=48 * 1024 * 1024
        ),
    )(velocity)
    any_space = pl.BlockSpec(memory_space=pl.ANY)
    local = pl.BlockSpec(memory_space=vmem)
    mag, one, two, three, four, five = pl.pallas_call(
        finish,
        name="finish",
        out_shape=(
            jax.ShapeDtypeStruct((12, 32, 2048), F32),
            jax.ShapeDtypeStruct((16, 48, 1024), F32),
            jax.ShapeDtypeStruct((8, 24, 512), F32),
            jax.ShapeDtypeStruct((12, 4, 256), F32),
            jax.ShapeDtypeStruct((6, 2, 128), F32),
            jax.ShapeDtypeStruct((3, 1, 64), F32),
        ),
        in_specs=[local, local],
        out_specs=(any_space, any_space, local, local, local, local),
        scratch_shapes=[
            vmem((4, 48, 128), F32),
            vmem((24, 128), F32),
            vmem((12, 128), F32),
            vmem((6, 128), F32),
            vmem((4, 12, 256), F32),
            vmem((2, 6, 128), F32),
            dma((2, 4)),
        ],
        compiler_params=pltpu.CompilerParams(vmem_limit_bytes=16 * 1024 * 1024),
    )(pltpu.with_memory_space_constraint(pencil, vmem), pltpu.with_memory_space_constraint(level, vmem))
    swap = lambda value: jnp.swapaxes(value, 0, 1)
    return swap(mag), one, two, swap(three), swap(four), swap(five)


def solution(mesh):
    in_specs = (P(None, "gx", "gy", "gz"),)
    out_specs = (
        P("gx", ("gy", "gz"), None),
        P("gx", "gy", None),
        P("gx", "gy", None),
        P("gx", "gy", None),
        P("gx", "gy", None),
        P("gx", "gy", None),
    )
    return jax.shard_map(
        on_device, mesh=mesh, in_specs=in_specs, out_specs=out_specs, check_vma=False
    )
```
